32 devices in a mesh: tile: 8 (over y, x, core), trc: 4 (over z).
Axes of the slice: x: 2, y: 2, z: 4, core: 2. Of those that a mesh axis runs over, the one named last changes fastest.
Arguments:
- tracers: float32 [512, 32, 2, 128], P('trc', 'tile'), may hold values from 0.05 to 2
- courant: float32 [3, 32, 2, 128], P(None, 'tile', None, 'trc'), may hold values from -6 to 6
- shear: float32 [3, 32, 2, 128], P(None, 'tile', None, 'trc'), may hold values from -8 to 8
- offsets: int32 [3, 32, 2, 128], P(None, 'tile'), may hold values from -1 to 0
- seam_flips: int32 [8], replicated, may hold values from 0 to 1
- kernel: float32 [32, 32], replicated, may hold values from 0.0005 to 0.004
- coag_target: int32 [32, 32], replicated, may hold values from 0 to 31, as said below
Outputs:
- updated: float32 [512, 32, 2, 128], P('trc', 'tile')
The draws below stay inside these ranges and needn't reach their ends.
Inputs may be any that keep to these rules, and one draw needn't show every extreme that they name: coag_target[i, j] lies between max(i, j) and 31.
All inputs are finite; a program needn't handle non-finite values.
Results may differ from the reference program's by a relative error of at most 0.00014.
Values sent between devices are 32-bit elements; how exact they have to be, the bound alone decides.
No kernel may reach another device: no remote copies, remote signals or barrier semaphores. Data moves between devices by JAX's collectives and lax.ppermute only.
A program may use at most 64 MiB of HBM per device.

```python
import math
import jax
import jax.numpy as jnp
from jax import lax

BINS = 32
COMPS = 16
ITER = 3
XW = 4
LEV = 2
YW = 128
TRACERS = 512
NX = 32
N_TILE = 8


def draw_coag_target(key, part):
    bin_index = jnp.arange(BINS, dtype=jnp.int32)
    floor_bin = jnp.maximum(bin_index[:, None], bin_index[None, :])
    return floor_bin + jax.random.randint(key, (BINS, BINS), 0, BINS - floor_bin)


def set_ends(drawn, rng, smallest, largest):
    longest = drawn.shape.index(max(drawn.shape))
    spots = []
    for shift in (0, 1):
        where = [jax.random.randint(jax.random.fold_in(rng, axis), (), 0, length) for axis, length in enumerate(drawn.shape)]
        where[longest] = (where[longest] + shift) % drawn.shape[longest]
        spots.append(tuple(where))
    return drawn.at[spots[0]].set(smallest).at[spots[1]].set(largest)


def level_of(own_key, dims, shards, low, largest):
    factor_of = 1.0
    for axis_at, shards_of in shards:
        heights = jax.random.uniform(jax.random.fold_in(jax.random.fold_in(own_key, 6), axis_at), (shards_of,), jnp.float32, low / len(shards), largest / len(shards))
        factor_of = factor_of * jnp.repeat(jnp.exp(heights), dims[axis_at] // shards_of).reshape((-1,) + (1,) * (len(dims) - 1 - axis_at))
    return factor_of


def gaussian(stream_key, extent, spread, reach, pieces=(), kind=jnp.bfloat16):
    drawn = spread * jax.random.normal(stream_key, extent, jnp.float32)
    if pieces:
        drawn = drawn * level_of(stream_key, extent, pieces, -0.22, 0.18)
    return jnp.clip(drawn, -reach, reach).astype(kind)


def setup_inputs(seed: int = 0) -> dict:
    keys = jax.random.split(jax.random.key(seed), 8)
    return {
        "tracers": jnp.clip(jnp.exp(math.log(2.0) - 3.6888794 * jax.random.uniform(keys[0], (TRACERS, NX, LEV, YW), jnp.float32) ** level_of(keys[0], (TRACERS, NX, LEV, YW), ((0, 4), (1, 8)), -0.2, 0.2)), 0.05, 2.0),
        "courant": gaussian(keys[1], (3, NX, LEV, YW), 1.5, 6.0, ((1, 8), (3, 4)), jnp.float32),
        "shear": gaussian(keys[2], (3, NX, LEV, YW), 2.0, 8.0, ((1, 8), (3, 4)), jnp.float32),
        "offsets": set_ends(jax.random.randint(keys[3], (3, NX, LEV, YW), -1, 1), jax.random.fold_in(keys[3], 1), -1, 0).astype(jnp.int32),
        "seam_flips": set_ends(jax.random.randint(keys[4], (N_TILE,), 0, 2), jax.random.fold_in(keys[4], 1), 0, 1).astype(jnp.int32),
        "kernel": jnp.clip(jnp.exp(jax.random.uniform(keys[5], (BINS, BINS), jnp.float32, math.log(0.0005), math.log(0.004))), 0.0005, 0.004),
        "coag_target": draw_coag_target(jax.random.fold_in(keys[7], 71), 0),
    }


precise = lax.Precision.HIGHEST


def fractions(courant, shear):
    fraction = jnp.full(courant.shape, 0.5, jnp.float32)
    for repeat in range(ITER):
        fraction = jax.nn.sigmoid(courant + shear * (fraction - 0.5))
    return fraction


def cubic_taps(fraction, offsets):
    first_node = -fraction * (fraction - 1.0) * (fraction - 2.0) / 6.0
    second_node = (fraction + 1.0) * (fraction - 1.0) * (fraction - 2.0) / 2.0
    third_node = -(fraction + 1.0) * fraction * (fraction - 2.0) / 2.0
    fourth_node = (fraction + 1.0) * fraction * (fraction - 1.0) / 6.0
    zeros = jnp.zeros_like(fraction)
    lower = offsets == -1
    weights = [jnp.where(lower, first_node, zeros), jnp.where(lower, second_node, first_node),
               jnp.where(lower, third_node, second_node), jnp.where(lower, fourth_node, third_node),
               jnp.where(lower, zeros, fourth_node)]
    return jnp.stack(weights, axis=1)


def interpolate(padded, stencil):
    cross, levels, along = stencil.shape[2], stencil.shape[3], stencil.shape[4]
    summed = jnp.zeros((padded.shape[0], cross, levels, along), jnp.float32)
    for x_step in range(5):
        for l_step in range(5):
            partial_sum = jnp.zeros((padded.shape[0], cross, levels, along), jnp.float32)
            for y_step in range(5):
                partial_sum = partial_sum + stencil[2, y_step] * padded[:, x_step:x_step + cross, l_step:l_step + levels, y_step:y_step + along]
            summed = summed + (stencil[0, x_step] * stencil[1, l_step]) * partial_sum
    return summed


def seam_pad(stacked, seam_flips):
    left_rim = jnp.roll(stacked, 1, axis=0)[:, :, -2:]
    right_rim = jnp.roll(stacked, -1, axis=0)[:, :, :2]
    left_flag = (seam_flips == 1)[:, None, None, None, None]
    right_flag = (jnp.roll(seam_flips, -1) == 1)[:, None, None, None, None]
    left_rim = jnp.where(left_flag, left_rim[..., ::-1], left_rim)
    right_rim = jnp.where(right_flag, right_rim[..., ::-1], right_rim)
    widened = jnp.concatenate([left_rim, stacked, right_rim], axis=2)
    widened = jnp.pad(widened, ((0, 0), (0, 0), (0, 0), (2, 2), (0, 0)), mode="edge")
    return jnp.pad(widened, ((0, 0), (0, 0), (0, 0), (0, 0), (2, 2)), mode="wrap")


def coagulate(masses, kernel, coag_target):
    number = jnp.sum(jnp.abs(masses), axis=1)
    losses = jnp.dot(kernel, number, precision=precise, preferred_element_type=jnp.float32)
    bin_index = jnp.arange(BINS, dtype=jnp.int32)
    matches = (coag_target[None, :, :] == bin_index[:, None, None]).astype(jnp.float32)
    redistribute = (matches * kernel[None, :, :]).reshape(BINS * BINS, BINS)
    transfer_rate = jnp.dot(redistribute, number, precision=precise, preferred_element_type=jnp.float32)
    transfer_rate = transfer_rate.reshape(BINS, BINS, number.shape[1])
    gained = jnp.einsum("bic,ikc->bkc", transfer_rate, masses, precision=precise)
    return (masses + gained) / (1.0 + losses[:, None, :])


def reference(tracers, courant, shear, offsets, seam_flips, kernel, coag_target):
    stencil = cubic_taps(fractions(courant, shear), offsets)
    stencil = stencil.reshape(3, 5, N_TILE, XW, LEV, YW).transpose(2, 0, 1, 3, 4, 5)
    stacked = tracers.reshape(TRACERS, N_TILE, XW, LEV, YW).transpose(1, 0, 2, 3, 4)

    def one_tile(operands):
        return interpolate(operands[0], operands[1])

    for repeat in range(2):
        padded = seam_pad(stacked, seam_flips)
        stacked = lax.map(one_tile, (padded, stencil))
    masses = stacked.reshape(N_TILE, BINS, COMPS, XW * LEV * YW)

    def one_block(block):
        return coagulate(block, kernel, coag_target)

    masses = lax.map(one_block, masses)
    masses = masses.reshape(N_TILE, TRACERS, XW, LEV, YW).transpose(1, 0, 2, 3, 4)
    return masses.reshape(TRACERS, NX, LEV, YW)
```

```python
import functools

import jax
import jax.numpy as jnp
from jax import lax
from jax.experimental import pallas as pl
from jax.experimental.pallas import tpu as pltpu
from jax.sharding import PartitionSpec as P

BINS = 32
COMPS = 16
ITER = 3
REACH = 2
SUB = 8
VMEM = pltpu.VMEM
SMEM = pltpu.SMEM


def shift(value, axis, step):
    count = lax.axis_size(axis)
    return lax.ppermute(value, axis, [(i, (i + step) % count) for i in range(count)])


def fractions(courant, shear):
    fraction = jnp.full(courant.shape, 0.5, jnp.float32)
    for _ in range(ITER):
        fraction = jax.nn.sigmoid(courant + shear * (fraction - 0.5))
    return fraction


def taps_of(fraction, lower):
    nodes = [
        -fraction * (fraction - 1.0) * (fraction - 2.0) / 6.0,
        (fraction + 1.0) * (fraction - 1.0) * (fraction - 2.0) / 2.0,
        -(fraction + 1.0) * fraction * (fraction - 2.0) / 2.0,
        (fraction + 1.0) * fraction * (fraction - 1.0) / 6.0,
    ]
    zeros = jnp.zeros_like(fraction)
    below = nodes + [zeros]
    above = [zeros] + nodes
    return [jnp.where(lower, p, q) for p, q in zip(below, above)]


def reversed_if(flag, value):
    lanes = value.shape[1]
    lane = lax.broadcasted_iota(jnp.int32, (SUB, lanes), 1)
    index = jnp.where(flag, lanes - 1 - lane, lane)
    return jnp.take_along_axis(value, index, axis=1)


def transport_kernel(dims, flips_ref, small_ref, own_ref, left_ref, right_ref, *rest):
    cross, levels, along, groups, parts = dims
    rows = cross * levels
    edge = REACH * levels
    wide = rows + 2 * edge
    outs = rest[:-4]
    weights, raw, once, final = rest[-4:]
    tile = lax.axis_index("tile")
    tiles = lax.axis_size("tile")
    spot = lax.axis_index("trc")
    flip_left = flips_ref[tile] == 1
    flip_right = flips_ref[lax.rem(tile + 1, tiles)] == 1
    chunk = along // lax.axis_size("trc")

    small = pltpu.roll(small_ref[...], (spot + 1) * chunk, 1)
    pieces = [small[k : k + SUB] for k in range(0, small.shape[0], SUB)]
    left_turn = jnp.concatenate([reversed_if(flip_left, p) for p in pieces], axis=0)
    right_turn = jnp.concatenate([reversed_if(flip_right, p) for p in pieces], axis=0)
    row = lax.broadcasted_iota(jnp.int32, (wide, along), 0)
    in_left = row < edge
    in_right = row >= wide - edge
    turned = (in_left & flip_left) | (in_right & flip_right)
    level = lax.rem(row, levels)

    def piece(k):
        part = slice(k * wide, (k + 1) * wide)
        return jnp.where(in_left, left_turn[part], jnp.where(in_right, right_turn[part], small[part]))

    taps = [taps_of(piece(d), piece(3 + d) < -0.5) for d in range(3)]
    count = 2 * REACH + 1
    for b in range(count):
        weights[b] = jnp.where(turned, taps[2][count - 1 - b], taps[2][b])
    for l in range(levels):
        share = jnp.zeros((wide, along), jnp.float32)
        for c in range(count):
            source = jnp.clip(level + (c - REACH), 0, levels - 1)
            share = share + jnp.where(source == l, taps[1][c], 0.0)
        for a in range(count):
            weights[count + a * levels + l] = taps[0][a] * share

    def spread(store, at, value):
        for b in range(count):
            back = (REACH - b) % along
            store[b, at] = value if back == 0 else pltpu.roll(value, back, 1)

    def combine(store, first, at):
        totals = [None] * levels
        for a in range(count):
            for l in range(levels):
                values = [store[b, (first + a) * levels + l] for b in range(count)]
                for o in range(levels):
                    r = at + o
                    inner = weights[0, r : r + 1] * values[0]
                    for b in range(1, count):
                        inner = inner + weights[b, r : r + 1] * values[b]
                    k = count + a * levels + l
                    term = weights[k, r : r + 1] * inner
                    totals[o] = term if totals[o] is None else totals[o] + term
        return totals

    def group(i, carry):
        base = i * (SUB * rows)
        for side, (ref, flag) in enumerate(((left_ref, flip_left), (own_ref, None), (right_ref, flip_right))):
            for j in range(rows):
                value = ref[pl.ds(base + j, SUB, rows), :]
                if flag is not None:
                    value = reversed_if(flag, value)
                spread(raw, side * rows + j, value)
        for x in range(cross + 2 * REACH):
            for l, value in enumerate(combine(raw, x + cross - 2 * REACH, x * levels)):
                spread(once, x * levels + l, value)
        for x in range(cross):
            for l, value in enumerate(combine(once, x, (x + REACH) * levels)):
                final[x * levels + l, pl.ds(pl.multiple_of(i * SUB, SUB), SUB), :] = value
        return carry

    lax.fori_loop(0, groups, group, 0)
    if len(outs) == 1:
        outs[0][...] = final[...]
    else:
        each = rows // parts
        for s in range(parts):
            start = lax.rem(spot + s, parts) * each
            outs[s][...] = final[pl.ds(start, each)]


def transported(small, own, left, right, flips, cross, levels, parts):
    tracers = own.shape[0] // (cross * levels)
    along = own.shape[1]
    rows = cross * levels
    wide = rows + 2 * REACH * levels
    count = 2 * REACH + 1
    split = rows % parts == 0
    shapes = [(rows // parts, tracers, along)] * parts if split else [(rows, tracers, along)]
    dims = (cross, levels, along, tracers // SUB, parts)
    return pl.pallas_call(
        functools.partial(transport_kernel, dims),
        out_shape=[jax.ShapeDtypeStruct(s, jnp.float32) for s in shapes],
        in_specs=[pl.BlockSpec(memory_space=SMEM)] + [pl.BlockSpec(memory_space=VMEM)] * 4,
        out_specs=[pl.BlockSpec(memory_space=VMEM)] * len(shapes),
        scratch_shapes=[
            VMEM((count * (1 + levels), wide, along), jnp.float32),
            VMEM((count, 3 * rows, SUB, along), jnp.float32),
            VMEM((count, wide, SUB, along), jnp.float32),
            VMEM((rows, tracers, along), jnp.float32),
        ],
        name="transport",
    )(flips, small, own, left, right)


def three_way(value):
    first = value.astype(jnp.bfloat16).astype(jnp.float32)
    second = (value - first).astype(jnp.bfloat16).astype(jnp.float32)
    return first, second, value - first - second


def rates_kernel(kernel_ref, target_ref, out_ref):
    k1, k2, k3 = three_way(kernel_ref[...])
    rate = jnp.concatenate([k1, k1, k2, k2, k1, k3], axis=1)
    target = jnp.concatenate([target_ref[...]] * 6, axis=1)
    for b in range(BINS):
        out_ref[pl.ds(b * BINS, BINS), :] = jnp.where(target == b, rate, 0.0).astype(jnp.bfloat16)
    out_ref[pl.ds(BINS * BINS, BINS), :] = rate.astype(jnp.bfloat16)


def rate_table(kernel, target):
    return pl.pallas_call(
        rates_kernel,
        out_shape=jax.ShapeDtypeStruct(((BINS + 1) * BINS, 6 * BINS), jnp.bfloat16),
        in_specs=[pl.BlockSpec(memory_space=VMEM)] * 2,
        out_specs=pl.BlockSpec(memory_space=VMEM),
        name="rates",
    )(kernel, target)


def coagulate_kernel(parts, rates_ref, *rest):
    blocks, outs = rest[:parts], rest[parts : 2 * parts]
    masses, number, transfer, result = rest[2 * parts :]
    spot = lax.axis_index("trc")
    _, each, tracers, lanes = masses.shape
    held = tracers // COMPS
    for s in range(parts):
        masses[lax.rem(spot + parts - s, parts)] = blocks[s][...]

    def mass(r, b, h):
        return masses[b // held, r, pl.ds((b % held) * COMPS + h * SUB, SUB), :]

    halves = COMPS // SUB
    for r in range(each):
        for b in range(BINS):
            total = jnp.abs(mass(r, b, 0))
            for h in range(1, halves):
                total = total + jnp.abs(mass(r, b, h))
            number[pl.ds(b, 1), pl.ds(r * lanes, lanes)] = jnp.sum(total, axis=0, keepdims=True)
    n1, n2, n3 = three_way(number[...])
    stacked = jnp.concatenate([n1, n2, n1, n2, n3, n1], axis=0).astype(jnp.bfloat16)
    transfer[...] = jnp.dot(rates_ref[...], stacked, preferred_element_type=jnp.float32)
    tail = pl.ds(BINS * BINS, BINS)
    transfer[tail, :] = 1.0 / (1.0 + transfer[tail, :])
    block = 4
    for r in range(each):
        lane = pl.ds(r * lanes, lanes)
        for first in range(0, BINS, block):
            bins = range(first, min(first + block, BINS))
            sums = {(b, h): mass(r, b, h) for b in bins for h in range(halves)}
            for i in range(bins[-1] + 1):
                source = [mass(r, i, h) for h in range(halves)]
                for b in bins:
                    if i <= b:
                        rate = transfer[pl.ds(b * BINS + i, 1), lane]
                        for h in range(halves):
                            sums[b, h] = sums[b, h] + rate * source[h]
            for b in bins:
                scale = transfer[pl.ds(BINS * BINS + b, 1), lane]
                for h in range(halves):
                    result[b // held, r, pl.ds((b % held) * COMPS + h * SUB, SUB), :] = sums[b, h] * scale
    for s in range(parts):
        outs[s][...] = result[lax.rem(spot + s, parts)]


def coagulated(rates, blocks):
    parts = len(blocks)
    each, tracers, lanes = blocks[0].shape
    shape = jax.ShapeDtypeStruct(blocks[0].shape, jnp.float32)
    return pl.pallas_call(
        functools.partial(coagulate_kernel, parts),
        out_shape=[shape] * parts,
        in_specs=[pl.BlockSpec(memory_space=VMEM)] * (parts + 1),
        out_specs=[pl.BlockSpec(memory_space=VMEM)] * parts,
        scratch_shapes=[
            VMEM((parts, each, tracers, lanes), jnp.float32),
            VMEM((BINS, each * lanes), jnp.float32),
            VMEM(((BINS + 1) * BINS, each * lanes), jnp.float32),
            VMEM((parts, each, tracers, lanes), jnp.float32),
        ],
        name="coagulate",
    )(rates, *blocks)


def collect_kernel(parts, *rest):
    blocks, out_ref, held = rest[:parts], rest[parts], rest[parts + 1]
    each, tracers, _ = blocks[0].shape
    rows = each * parts
    spot = lax.axis_index("trc")
    for s in range(parts):
        held[pl.ds(lax.rem(spot + parts - s, parts) * each, each)] = blocks[s][...]
    for i in range(tracers // SUB):
        for r in range(rows):
            out_ref[pl.ds(i * SUB * rows + r, SUB, rows), :] = held[r, pl.ds(i * SUB, SUB), :]


def collected(blocks):
    parts = len(blocks)
    each, tracers, along = blocks[0].shape
    rows = each * parts
    return pl.pallas_call(
        functools.partial(collect_kernel, parts),
        out_shape=jax.ShapeDtypeStruct((tracers * rows, along), jnp.float32),
        in_specs=[pl.BlockSpec(memory_space=VMEM)] * parts,
        out_specs=pl.BlockSpec(memory_space=VMEM),
        scratch_shapes=[VMEM((rows, tracers, along), jnp.float32)],
        name="collect",
    )(*blocks)


def on_device(tracers, courant, shear, offsets, seam_flips, kernel, coag_target):
    held, cross, levels, along = tracers.shape
    rows = cross * levels
    parts = lax.axis_size("trc")
    spot = lax.axis_index("trc")
    chunk = along // parts
    edge = REACH * levels

    own_offsets = lax.dynamic_slice_in_dim(offsets, spot * chunk, chunk, 3)
    small = jnp.concatenate([fractions(courant, shear), own_offsets.astype(jnp.float32)], axis=0)
    small = small.reshape(6, rows, chunk)
    below = shift(small[:, rows - edge :], "tile", 1)
    above = shift(small[:, :edge], "tile", -1)
    left = shift(tracers, "tile", 1)
    right = shift(tracers, "tile", -1)
    small = jnp.concatenate([below, small, above], axis=1).reshape(-1, chunk)
    strips = [shift(small, "trc", s) for s in range(parts - 1, 0, -1)] + [small]
    small = jnp.concatenate(strips, axis=1)
    rates = rate_table(kernel, coag_target)

    flat = (held * rows, along)
    blocks = transported(
        small, tracers.reshape(flat), left.reshape(flat), right.reshape(flat), seam_flips, cross, levels, parts
    )
    if len(blocks) == 1:
        lanes = rows * along // parts
        cells = blocks[0].reshape(rows, held, along // lanes, lanes).transpose(0, 2, 1, 3)
        cells = jnp.roll(cells.reshape(parts, 1, held, lanes), -spot, axis=0)
        blocks = [cells[s] for s in range(parts)]
    blocks = [blocks[0]] + [shift(blocks[s], "trc", s) for s in range(1, parts)]
    blocks = coagulated(rates, blocks)
    blocks = [blocks[0]] + [shift(blocks[s], "trc", s) for s in range(1, parts)]
    if rows % parts == 0:
        return collected(blocks).reshape(tracers.shape)
    lanes = blocks[0].shape[-1]
    cells = jnp.stack([blocks[0]] + blocks[:0:-1], axis=0)
    cells = jnp.roll(cells, spot, axis=0).reshape(rows, along // lanes, held, lanes)
    return cells.transpose(2, 0, 1, 3).reshape(tracers.shape)


def solution(mesh):
    placed = (
        P("trc", "tile", None, None),
        P(None, "tile", None, "trc"),
        P(None, "tile", None, "trc"),
        P(None, "tile", None, None),
        P(),
        P(),
        P(),
    )
    return jax.shard_map(
        on_device,
        mesh=mesh,
        in_specs=placed,
        out_specs=P("trc", "tile", None, None),
        check_vma=False,
    )
```

```python
import functools

import jax
import jax.numpy as jnp
from jax import lax
from jax.experimental import pallas as pl
from jax.experimental.pallas import tpu as pltpu
from jax.sharding import PartitionSpec as P


BINS = 32
COMPS = 16
ITER = 3
BATCHES = 2
REACH = 2
SUB = 8
VMEM = pltpu.VMEM
SMEM = pltpu.SMEM


def near(value):
    return pltpu.with_memory_space_constraint(value, VMEM)


def shift(value, axis, step):
    count = lax.axis_size(axis)
    return lax.ppermute(value, axis, [(i, (i + step) % count) for i in range(count)])


def doubling(count):
    return count & (count - 1) == 0


def target(spot, step, count):
    return spot ^ step if doubling(count) else lax.rem(spot + step, count)


def source(spot, step, count):
    return spot ^ step if doubling(count) else lax.rem(spot + count - step, count)


def trade(value, axis, step):
    count = lax.axis_size(axis)
    if doubling(count):
        return lax.ppermute(value, axis, [(i, i ^ step) for i in range(count)])
    return shift(value, axis, step)


def fractions(courant, shear):
    fraction = jnp.full(courant.shape, 0.5, jnp.float32)
    for _ in range(ITER):
        fraction = jax.nn.sigmoid(courant + shear * (fraction - 0.5))
    return fraction


def taps_of(fraction, lower):
    nodes = [
        -fraction * (fraction - 1.0) * (fraction - 2.0) / 6.0,
        (fraction + 1.0) * (fraction - 1.0) * (fraction - 2.0) / 2.0,
        -(fraction + 1.0) * fraction * (fraction - 2.0) / 2.0,
        (fraction + 1.0) * fraction * (fraction - 1.0) / 6.0,
    ]
    zeros = jnp.zeros_like(fraction)
    below = nodes + [zeros]
    above = [zeros] + nodes
    return [jnp.where(lower, p, q) for p, q in zip(below, above)]


def lane_of(flag, lanes):
    lane = lax.broadcasted_iota(jnp.int32, (SUB, lanes), 1)
    return jnp.where(flag, lanes - 1 - lane, lane)


def reversed_if(flag, value):
    return jnp.take_along_axis(value, lane_of(flag, value.shape[1]), axis=1)


def transport_kernel(dims, flips_ref, small_ref, own_ref, left_ref, right_ref, *rest):
    cross, levels, along, groups, parts, skip = dims
    rows = cross * levels
    edge = REACH * levels
    wide = rows + 2 * edge
    outs = rest[:-4]
    weights, raw, once, final = rest[-4:]
    tile = lax.axis_index("tile")
    tiles = lax.axis_size("tile")
    spot = lax.axis_index("trc")
    flip_left = flips_ref[tile] == 1
    flip_right = flips_ref[lax.rem(tile + 1, tiles)] == 1
    chunk = along // parts

    def unscrambled(flag):
        lane = lane_of(flag, along)
        index = source(spot, lax.div(lane, chunk), parts) * chunk + lax.rem(lane, chunk)
        pieces = [small_ref[k : k + SUB] for k in range(0, small_ref.shape[0], SUB)]
        return jnp.concatenate([jnp.take_along_axis(p, index, axis=1) for p in pieces], axis=0)

    small, left_turn, right_turn = unscrambled(False), unscrambled(flip_left), unscrambled(flip_right)
    row = lax.broadcasted_iota(jnp.int32, (wide, along), 0)
    in_left = row < edge
    in_right = row >= wide - edge
    turned = (in_left & flip_left) | (in_right & flip_right)
    level = lax.rem(row, levels)

    def piece(k):
        part = slice(k * wide, (k + 1) * wide)
        return jnp.where(in_left, left_turn[part], jnp.where(in_right, right_turn[part], small[part]))

    taps = [taps_of(piece(d), piece(3 + d) < -0.5) for d in range(3)]
    count = 2 * REACH + 1
    for b in range(count):
        weights[b] = jnp.where(turned, taps[2][count - 1 - b], taps[2][b])
    for l in range(levels):
        share = jnp.zeros((wide, along), jnp.float32)
        for c in range(count):
            read = jnp.clip(level + (c - REACH), 0, levels - 1)
            share = share + jnp.where(read == l, taps[1][c], 0.0)
        for a in range(count):
            weights[count + a * levels + l] = taps[0][a] * share

    def spread(store, at, value):
        for b in range(count):
            back = (REACH - b) % along
            store[b, at] = value if back == 0 else pltpu.roll(value, back, 1)

    def combine(store, first, at):
        totals = [None] * levels
        for a in range(count):
            for l in range(levels):
                values = [store[b, (first + a) * levels + l] for b in range(count)]
                for o in range(levels):
                    r = at + o
                    inner = weights[0, r : r + 1] * values[0]
                    for b in range(1, count):
                        inner = inner + weights[b, r : r + 1] * values[b]
                    k = count + a * levels + l
                    term = weights[k, r : r + 1] * inner
                    totals[o] = term if totals[o] is None else totals[o] + term
        return totals

    def group(i, carry):
        base = i * (SUB * rows)
        for side, (ref, flag) in enumerate(((left_ref, flip_left), (own_ref, None), (right_ref, flip_right))):
            for j in range(rows):
                value = ref[pl.ds(base + (skip * rows if side == 1 else 0) + j, SUB, rows), :]
                if flag is not None:
                    value = reversed_if(flag, value)
                spread(raw, side * rows + j, value)
        for x in range(cross + 2 * REACH):
            for l, value in enumerate(combine(raw, x + cross - 2 * REACH, x * levels)):
                spread(once, x * levels + l, value)
        for x in range(cross):
            for l, value in enumerate(combine(once, x, (x + REACH) * levels)):
                final[x * levels + l, pl.ds(pl.multiple_of(i * SUB, SUB), SUB), :] = value
        return carry

    lax.fori_loop(0, groups, group, 0)
    if len(outs) == 1:
        outs[0][...] = final[...]
    else:
        each = rows // parts
        for s in range(parts):
            start = target(spot, s, parts) * each
            outs[s][...] = final[pl.ds(start, each)]


def transported(small, own, left, right, flips, cross, levels, parts, skip):
    tracers = left.shape[0] // (cross * levels)
    along = own.shape[1]
    rows = cross * levels
    wide = rows + 2 * REACH * levels
    count = 2 * REACH + 1
    split = rows % parts == 0
    shapes = [(rows // parts, tracers, along)] * parts if split else [(rows, tracers, along)]
    dims = (cross, levels, along, tracers // SUB, parts, skip)
    return pl.pallas_call(
        functools.partial(transport_kernel, dims),
        out_shape=[VMEM(s, jnp.float32) for s in shapes],
        in_specs=[pl.BlockSpec(memory_space=SMEM)] + [pl.BlockSpec(memory_space=VMEM)] * 4,
        out_specs=[pl.BlockSpec(memory_space=VMEM)] * len(shapes),
        scratch_shapes=[
            VMEM((count * (1 + levels), wide, along), jnp.float32),
            VMEM((count, 3 * rows, SUB, along), jnp.float32),
            VMEM((count, wide, SUB, along), jnp.float32),
            VMEM((rows, tracers, along), jnp.float32),
        ],
        name="transport",
    )(flips, *map(near, (small, own, left, right)))


def three_way(value):
    first = value.astype(jnp.bfloat16).astype(jnp.float32)
    second = (value - first).astype(jnp.bfloat16).astype(jnp.float32)
    return first, second, value - first - second


def rates_kernel(kernel_ref, target_ref, out_ref):
    k1, k2, k3 = three_way(kernel_ref[...])
    rate = jnp.concatenate([k1, k1, k2, k2, k1, k3], axis=1)
    target = jnp.concatenate([target_ref[...]] * 6, axis=1)
    for b in range(BINS):
        out_ref[pl.ds(b * BINS, BINS), :] = jnp.where(target == b, rate, 0.0).astype(jnp.bfloat16)
    out_ref[pl.ds(BINS * BINS, BINS), :] = rate.astype(jnp.bfloat16)


def rate_table(kernel, target):
    return pl.pallas_call(
        rates_kernel,
        out_shape=VMEM(((BINS + 1) * BINS, 6 * BINS), jnp.bfloat16),
        in_specs=[pl.BlockSpec(memory_space=VMEM)] * 2,
        out_specs=pl.BlockSpec(memory_space=VMEM),
        name="rates",
    )(kernel, target)


def coagulate_kernel(parts, rates_ref, *rest):
    masses, number, transfer, result = rest[-4:]
    blocks, outs = rest[: -4 - parts], rest[-4 - parts : -4]
    spot = lax.axis_index("trc")
    _, each, tracers, lanes = masses.shape
    held = tracers // COMPS
    for at, block in enumerate(blocks):
        size = block.shape[1]
        masses[source(spot, at % parts, parts), :, pl.ds(at // parts * size, size)] = block[...]

    def mass(r, b, h):
        return masses[b // held, r, pl.ds((b % held) * COMPS + h * SUB, SUB), :]

    halves = COMPS // SUB
    for r in range(each):
        for b in range(BINS):
            total = jnp.abs(mass(r, b, 0))
            for h in range(1, halves):
                total = total + jnp.abs(mass(r, b, h))
            number[pl.ds(b, 1), pl.ds(r * lanes, lanes)] = jnp.sum(total, axis=0, keepdims=True)
    n1, n2, n3 = three_way(number[...])
    stacked = jnp.concatenate([n1, n2, n1, n2, n3, n1], axis=0).astype(jnp.bfloat16)
    transfer[...] = jnp.dot(rates_ref[...], stacked, preferred_element_type=jnp.float32)
    tail = pl.ds(BINS * BINS, BINS)
    transfer[tail, :] = 1.0 / (1.0 + transfer[tail, :])
    block = 4
    for r in range(each):
        lane = pl.ds(r * lanes, lanes)
        for first in range(0, BINS, block):
            bins = range(first, min(first + block, BINS))
            sums = {(b, h): mass(r, b, h) for b in bins for h in range(halves)}
            for i in range(bins[-1] + 1):
                inner = [mass(r, i, h) for h in range(halves)]
                for b in bins:
                    if i <= b:
                        rate = transfer[pl.ds(b * BINS + i, 1), lane]
                        for h in range(halves):
                            sums[b, h] = sums[b, h] + rate * inner[h]
            for b in bins:
                scale = transfer[pl.ds(BINS * BINS + b, 1), lane]
                for h in range(halves):
                    result[b // held, r, pl.ds((b % held) * COMPS + h * SUB, SUB), :] = sums[b, h] * scale
    for s in range(parts):
        outs[s][...] = result[target(spot, s, parts)]


def coagulated(rates, blocks, parts):
    each, size, lanes = blocks[0].shape
    tracers = size * (len(blocks) // parts)
    return pl.pallas_call(
        functools.partial(coagulate_kernel, parts),
        out_shape=[VMEM((each, tracers, lanes), jnp.float32)] * parts,
        in_specs=[pl.BlockSpec(memory_space=VMEM)] * (len(blocks) + 1),
        out_specs=[pl.BlockSpec(memory_space=VMEM)] * parts,
        scratch_shapes=[
            VMEM((parts, each, tracers, lanes), jnp.float32),
            VMEM((BINS, each * lanes), jnp.float32),
            VMEM(((BINS + 1) * BINS, each * lanes), jnp.float32),
            VMEM((parts, each, tracers, lanes), jnp.float32),
        ],
        name="coagulate",
    )(*map(near, (rates, *blocks)))


def collect_kernel(parts, *rest):
    blocks, out_ref, held = rest[:parts], rest[parts], rest[parts + 1]
    each, tracers, _ = blocks[0].shape
    rows = each * parts
    spot = lax.axis_index("trc")
    for s in range(parts):
        held[pl.ds(source(spot, s, parts) * each, each)] = blocks[s][...]
    for i in range(tracers // SUB):
        for r in range(rows):
            out_ref[pl.ds(i * SUB * rows + r, SUB, rows), :] = held[r, pl.ds(i * SUB, SUB), :]


def collected(blocks):
    parts = len(blocks)
    each, tracers, along = blocks[0].shape
    rows = each * parts
    return pl.pallas_call(
        functools.partial(collect_kernel, parts),
        out_shape=jax.ShapeDtypeStruct((tracers * rows, along), jnp.float32),
        in_specs=[pl.BlockSpec(memory_space=VMEM)] * parts,
        out_specs=pl.BlockSpec(memory_space=VMEM),
        scratch_shapes=[VMEM((rows, tracers, along), jnp.float32)],
        name="collect",
    )(*map(near, blocks))


def on_device(tracers, courant, shear, offsets, seam_flips, kernel, coag_target):
    held, cross, levels, along = tracers.shape
    rows = cross * levels
    parts = lax.axis_size("trc")
    spot = lax.axis_index("trc")
    chunk = along // parts
    edge = REACH * levels
    batches = BATCHES if held % (BATCHES * SUB) == 0 else 1
    size = held // batches

    own_offsets = lax.dynamic_slice_in_dim(offsets, spot * chunk, chunk, 3)
    small = jnp.concatenate([fractions(courant, shear), own_offsets.astype(jnp.float32)], axis=0)
    small = small.reshape(6, rows, chunk)
    below = shift(small[:, rows - edge :], "tile", 1)
    above = shift(small[:, :edge], "tile", -1)
    left, right = [], []
    for k in range(batches):
        batch = tracers[k * size : (k + 1) * size]
        left.append(shift(batch, "tile", 1))
        right.append(shift(batch, "tile", -1))
    small = jnp.concatenate([below, small, above], axis=1).reshape(-1, chunk)
    strips = [small]
    for s in range(1, parts):
        strips.append(trade(small, "trc", s))
    small = jnp.concatenate(strips, axis=1)
    rates = rate_table(kernel, coag_target)

    flat = (-1, along)
    own = tracers.reshape(flat)
    gathered = []
    for k in range(batches):
        blocks = transported(
            small, own, left[k].reshape(flat), right[k].reshape(flat), seam_flips, cross, levels, parts, k * size
        )
        if len(blocks) == 1:
            lanes = rows * along // parts
            cells = blocks[0].reshape(rows, size, along // lanes, lanes).transpose(0, 2, 1, 3)
            cells = cells.reshape(parts, 1, size, lanes)
            blocks = [lax.dynamic_index_in_dim(cells, target(spot, s, parts), 0, False) for s in range(parts)]
        gathered.append(blocks[0])
        for s in range(1, parts):
            gathered.append(trade(blocks[s], "trc", s))
    blocks = coagulated(rates, gathered, parts)
    returned = [blocks[0]]
    for s in range(1, parts):
        returned.append(trade(blocks[s], "trc", s))
    if rows % parts == 0:
        return collected(returned).reshape(tracers.shape)
    lanes = blocks[0].shape[-1]
    cells = jnp.stack(returned, axis=0)
    cells = cells[jnp.stack([source(spot, jnp.int32(c), parts) if doubling(parts) else lax.rem(spot - c + parts, parts) for c in range(parts)])]
    cells = cells.reshape(rows, along // lanes, held, lanes)
    return cells.transpose(2, 0, 1, 3).reshape(tracers.shape)


def solution(mesh):
    placed = (
        P("trc", "tile", None, None),
        P(None, "tile", None, "trc"),
        P(None, "tile", None, "trc"),
        P(None, "tile", None, None),
        P(),
        P(),
        P(),
    )

    return jax.shard_map(
        on_device,
        mesh=mesh,
        in_specs=placed,
        out_specs=P("trc", "tile", None, None),
        check_vma=False,
    )
```

```python
import functools

import jax
import jax.numpy as jnp
from jax import lax
from jax.experimental import pallas as pl
from jax.experimental.pallas import tpu as pltpu
from jax.sharding import PartitionSpec as P


BINS = 32
COMPS = 16
ITER = 3
BATCHES = 2
REACH = 2
SUB = 8
VMEM = pltpu.VMEM


def near(value):
    return pltpu.with_memory_space_constraint(value, VMEM)


def shift(value, axis, step):
    count = lax.axis_size(axis)
    return lax.ppermute(value, axis, [(i, (i + step) % count) for i in range(count)])


def doubling(count):
    return count & (count - 1) == 0


def target(spot, step, count):
    return spot ^ step if doubling(count) else lax.rem(spot + step, count)


def source(spot, step, count):
    return spot ^ step if doubling(count) else lax.rem(spot + count - step, count)


def trade(value, axis, step):
    count = lax.axis_size(axis)
    if doubling(count):
        return lax.ppermute(value, axis, [(i, i ^ step) for i in range(count)])
    return shift(value, axis, step)


def fractions(courant, shear):
    fraction = jnp.full(courant.shape, 0.5, jnp.float32)
    for _ in range(ITER):
        fraction = jax.nn.sigmoid(courant + shear * (fraction - 0.5))
    return fraction


def taps_of(fraction, lower):
    nodes = [
        -fraction * (fraction - 1.0) * (fraction - 2.0) / 6.0,
        (fraction + 1.0) * (fraction - 1.0) * (fraction - 2.0) / 2.0,
        -(fraction + 1.0) * fraction * (fraction - 2.0) / 2.0,
        (fraction + 1.0) * fraction * (fraction - 1.0) / 6.0,
    ]
    zeros = jnp.zeros_like(fraction)
    below = nodes + [zeros]
    above = [zeros] + nodes
    return [jnp.where(lower, p, q) for p, q in zip(below, above)]


def lane_of(flag, lanes):
    lane = lax.broadcasted_iota(jnp.int32, (SUB, lanes), 1)
    return jnp.where(flag, lanes - 1 - lane, lane)


def reversed_if(flag, value):
    return jnp.take_along_axis(value, lane_of(flag, value.shape[1]), axis=1)


def fill_weights(dims, flip_left, flip_right, small_ref, weights):
    cross, levels, along, _, parts, _ = dims
    edge = REACH * levels
    wide = cross * levels + 2 * edge
    spot = lax.axis_index("trc")
    chunk = along // parts

    def unscrambled(flag):
        lane = lane_of(flag, along)
        index = source(spot, lax.div(lane, chunk), parts) * chunk + lax.rem(lane, chunk)
        pieces = [small_ref[k : k + SUB] for k in range(0, small_ref.shape[0], SUB)]
        return jnp.concatenate([jnp.take_along_axis(p, index, axis=1) for p in pieces], axis=0)

    small, left_turn, right_turn = unscrambled(False), unscrambled(flip_left), unscrambled(flip_right)
    row = lax.broadcasted_iota(jnp.int32, (wide, along), 0)
    in_left = row < edge
    in_right = row >= wide - edge
    whole = [jnp.concatenate([f] * (wide // SUB), axis=0) for f in (flip_left, flip_right)]
    turned = (in_left & whole[0]) | (in_right & whole[1])
    level = lax.rem(row, levels)

    def piece(k):
        part = slice(k * wide, (k + 1) * wide)
        return jnp.where(in_left, left_turn[part], jnp.where(in_right, right_turn[part], small[part]))

    taps = [taps_of(piece(d), piece(3 + d) < -0.5) for d in range(3)]
    count = 2 * REACH + 1
    for b in range(count):
        weights[b] = jnp.where(turned, taps[2][count - 1 - b], taps[2][b])
    for l in range(levels):
        share = jnp.zeros((wide, along), jnp.float32)
        for c in range(count):
            read = jnp.clip(level + (c - REACH), 0, levels - 1)
            share = share + jnp.where(read == l, taps[1][c], 0.0)
        for a in range(count):
            weights[count + a * levels + l] = taps[0][a] * share


def transport_kernel(dims, first, flips_ref, small_ref, own_ref, left_ref, right_ref, *rest):
    cross, levels, along, groups, parts, skip = dims
    rows = cross * levels
    *outs, raw, once, final = rest
    spot = lax.axis_index("trc")
    flip_left = flips_ref[0:SUB] == 1
    flip_right = flips_ref[SUB : 2 * SUB] == 1
    count = 2 * REACH + 1
    if first:
        weights, *outs = outs
        fill_weights(dims, flip_left, flip_right, small_ref, weights)
    else:
        weights = small_ref

    def spread(store, at, value):
        for b in range(count):
            back = (REACH - b) % along
            store[b, at] = value if back == 0 else pltpu.roll(value, back, 1)

    def combine(store, first, at):
        totals = [None] * levels
        for a in range(count):
            for l in range(levels):
                values = [store[b, (first + a) * levels + l] for b in range(count)]
                for o in range(levels):
                    r = at + o
                    inner = weights[0, r : r + 1] * values[0]
                    for b in range(1, count):
                        inner = inner + weights[b, r : r + 1] * values[b]
                    k = count + a * levels + l
                    term = weights[k, r : r + 1] * inner
                    totals[o] = term if totals[o] is None else totals[o] + term
        return totals

    def group(i, carry):
        base = i * (SUB * rows)
        for side, (ref, flag) in enumerate(((left_ref, flip_left), (own_ref, None), (right_ref, flip_right))):
            for j in range(rows):
                value = ref[pl.ds(base + (skip * rows if side == 1 else 0) + j, SUB, rows), :]
                if flag is not None:
                    value = reversed_if(flag, value)
                spread(raw, side * rows + j, value)
        for x in range(cross + 2 * REACH):
            for l, value in enumerate(combine(raw, x + cross - 2 * REACH, x * levels)):
                spread(once, x * levels + l, value)
        for x in range(cross):
            for l, value in enumerate(combine(once, x, (x + REACH) * levels)):
                final[x * levels + l, pl.ds(pl.multiple_of(i * SUB, SUB), SUB), :] = value
        return carry

    lax.fori_loop(0, groups, group, 0)
    if len(outs) == 1:
        outs[0][...] = final[...]
    else:
        each = rows // parts
        for s in range(parts):
            start = target(spot, s, parts) * each
            outs[s][...] = final[pl.ds(start, each)]


def transported(stencil, own, left, right, flips, cross, levels, parts, skip):
    tracers = left.shape[0] // (cross * levels)
    along = own.shape[1]
    rows = cross * levels
    wide = rows + 2 * REACH * levels
    count = 2 * REACH + 1
    split = rows % parts == 0
    first = stencil.ndim == 2
    shapes = [(rows // parts, tracers, along)] * parts if split else [(rows, tracers, along)]
    kept = [(count * (1 + levels), wide, along)] if first else []
    dims = (cross, levels, along, tracers // SUB, parts, skip)
    found = pl.pallas_call(
        functools.partial(transport_kernel, dims, first),
        out_shape=[VMEM(s, jnp.float32) for s in kept + shapes],
        in_specs=[pl.BlockSpec(memory_space=VMEM)] * 5,
        out_specs=[pl.BlockSpec(memory_space=VMEM)] * len(kept + shapes),
        scratch_shapes=[
            VMEM((count, 3 * rows, SUB, along), jnp.float32),
            VMEM((count, wide, SUB, along), jnp.float32),
            VMEM((rows, tracers, along), jnp.float32),
        ],
        name="transport",
    )(*map(near, (flips, stencil, own, left, right)))
    return (found[0], found[1:]) if first else (stencil, found)


def three_way(value):
    first = value.astype(jnp.bfloat16).astype(jnp.float32)
    second = (value - first).astype(jnp.bfloat16).astype(jnp.float32)
    return first, second, value - first - second


def rates_kernel(kernel_ref, target_ref, out_ref):
    k1, k2, k3 = three_way(kernel_ref[...])
    rate = jnp.concatenate([k1, k1, k2, k2, k1, k3], axis=1)
    target = jnp.concatenate([target_ref[...]] * 6, axis=1)
    for b in range(BINS):
        out_ref[pl.ds(b * BINS, BINS), :] = jnp.where(target == b, rate, 0.0).astype(jnp.bfloat16)
    out_ref[pl.ds(BINS * BINS, BINS), :] = rate.astype(jnp.bfloat16)


def rate_table(kernel, target):
    return pl.pallas_call(
        rates_kernel,
        out_shape=VMEM(((BINS + 1) * BINS, 6 * BINS), jnp.bfloat16),
        in_specs=[pl.BlockSpec(memory_space=VMEM)] * 2,
        out_specs=pl.BlockSpec(memory_space=VMEM),
        name="rates",
    )(kernel, target)


def coagulate_kernel(parts, rates_ref, *rest):
    masses, number, transfer, result = rest[-4:]
    blocks, outs = rest[: -4 - parts], rest[-4 - parts : -4]
    spot = lax.axis_index("trc")
    _, each, tracers, lanes = masses.shape
    held = tracers // COMPS
    for at, block in enumerate(blocks):
        size = block.shape[1]
        masses[source(spot, at % parts, parts), :, pl.ds(at // parts * size, size)] = block[...]

    def mass(r, b, h):
        return masses[b // held, r, pl.ds((b % held) * COMPS + h * SUB, SUB), :]

    halves = COMPS // SUB
    for r in range(each):
        for b in range(BINS):
            total = jnp.abs(mass(r, b, 0))
            for h in range(1, halves):
                total = total + jnp.abs(mass(r, b, h))
            number[pl.ds(b, 1), pl.ds(r * lanes, lanes)] = jnp.sum(total, axis=0, keepdims=True)
    n1, n2, n3 = three_way(number[...])
    stacked = jnp.concatenate([n1, n2, n1, n2, n3, n1], axis=0).astype(jnp.bfloat16)
    transfer[...] = jnp.dot(rates_ref[...], stacked, preferred_element_type=jnp.float32)
    tail = pl.ds(BINS * BINS, BINS)
    transfer[tail, :] = 1.0 / (1.0 + transfer[tail, :])
    block = 4
    for r in range(each):
        lane = pl.ds(r * lanes, lanes)
        for first in range(0, BINS, block):
            bins = range(first, min(first + block, BINS))
            sums = {(b, h): mass(r, b, h) for b in bins for h in range(halves)}
            for i in range(bins[-1] + 1):
                inner = [mass(r, i, h) for h in range(halves)]
                for b in bins:
                    if i <= b:
                        rate = transfer[pl.ds(b * BINS + i, 1), lane]
                        for h in range(halves):
                            sums[b, h] = sums[b, h] + rate * inner[h]
            for b in bins:
                scale = transfer[pl.ds(BINS * BINS + b, 1), lane]
                for h in range(halves):
                    result[b // held, r, pl.ds((b % held) * COMPS + h * SUB, SUB), :] = sums[b, h] * scale
    for s in range(parts):
        outs[s][...] = result[target(spot, s, parts)]


def coagulated(rates, blocks, parts):
    each, size, lanes = blocks[0].shape
    tracers = size * (len(blocks) // parts)
    return pl.pallas_call(
        functools.partial(coagulate_kernel, parts),
        out_shape=[VMEM((each, tracers, lanes), jnp.float32)] * parts,
        in_specs=[pl.BlockSpec(memory_space=VMEM)] * (len(blocks) + 1),
        out_specs=[pl.BlockSpec(memory_space=VMEM)] * parts,
        scratch_shapes=[
            VMEM((parts, each, tracers, lanes), jnp.float32),
            VMEM((BINS, each * lanes), jnp.float32),
            VMEM(((BINS + 1) * BINS, each * lanes), jnp.float32),
            VMEM((parts, each, tracers, lanes), jnp.float32),
        ],
        name="coagulate",
    )(*map(near, (rates, *blocks)))


def collect_kernel(parts, *rest):
    blocks, out_ref, held = rest[:parts], rest[parts], rest[parts + 1]
    each, tracers, _ = blocks[0].shape
    rows = each * parts
    spot = lax.axis_index("trc")
    for s in range(parts):
        held[pl.ds(source(spot, s, parts) * each, each)] = blocks[s][...]
    for i in range(tracers // SUB):
        for r in range(rows):
            out_ref[pl.ds(i * SUB * rows + r, SUB, rows), :] = held[r, pl.ds(i * SUB, SUB), :]


def collected(blocks):
    parts = len(blocks)
    each, tracers, along = blocks[0].shape
    rows = each * parts
    return pl.pallas_call(
        functools.partial(collect_kernel, parts),
        out_shape=jax.ShapeDtypeStruct((tracers * rows, along), jnp.float32),
        in_specs=[pl.BlockSpec(memory_space=VMEM)] * parts,
        out_specs=pl.BlockSpec(memory_space=VMEM),
        scratch_shapes=[VMEM((rows, tracers, along), jnp.float32)],
        name="collect",
    )(*map(near, blocks))


def on_device(tracers, courant, shear, offsets, seam_flips, kernel, coag_target):
    held, cross, levels, along = tracers.shape
    rows = cross * levels
    parts = lax.axis_size("trc")
    spot = lax.axis_index("trc")
    chunk = along // parts
    edge = REACH * levels
    batches = BATCHES if held % (BATCHES * SUB) == 0 else 1
    size = held // batches

    own_offsets = lax.dynamic_slice_in_dim(offsets, spot * chunk, chunk, 3)
    small = jnp.concatenate([fractions(courant, shear), own_offsets.astype(jnp.float32)], axis=0)
    small = small.reshape(6, rows, chunk)
    below = shift(small[:, rows - edge :], "tile", 1)
    above = shift(small[:, :edge], "tile", -1)
    wings = [below, above]
    left, right = [], []
    early = tracers[:size]
    for k in range(batches):
        if k == 1:
            wings, late = lax.optimization_barrier((wings, tracers))
        batch = early if k == 0 else late[k * size : (k + 1) * size]
        left.append(shift(batch, "tile", 1))
        right.append(shift(batch, "tile", -1))
    small = jnp.concatenate([wings[0], small, wings[1]], axis=1).reshape(-1, chunk)
    strips = [small]
    for s in range(1, parts):
        strips.append(trade(small, "trc", s))
    small = jnp.concatenate(strips, axis=1)
    rates = rate_table(kernel, coag_target)

    tile = lax.axis_index("tile")
    ends = jnp.stack([tile, lax.rem(tile + 1, lax.axis_size("tile"))])
    flips = jnp.broadcast_to(jnp.repeat(seam_flips[ends], SUB)[:, None], (2 * SUB, along))
    flat = (-1, along)
    stencil = small
    own = tracers.reshape(flat)
    gathered = []
    for k in range(batches):
        stencil, blocks = transported(
            stencil, own, left[k].reshape(flat), right[k].reshape(flat), flips, cross, levels, parts, k * size
        )
        if len(blocks) == 1:
            lanes = rows * along // parts
            cells = blocks[0].reshape(rows, size, along // lanes, lanes).transpose(0, 2, 1, 3)
            cells = cells.reshape(parts, 1, size, lanes)
            blocks = [lax.dynamic_index_in_dim(cells, target(spot, s, parts), 0, False) for s in range(parts)]
        gathered.append(blocks[0])
        for s in range(1, parts):
            gathered.append(trade(blocks[s], "trc", s))
    blocks = coagulated(rates, gathered, parts)
    returned = [blocks[0]]
    for s in range(1, parts):
        returned.append(trade(blocks[s], "trc", s))
    if rows % parts == 0:
        return collected(returned).reshape(tracers.shape)
    lanes = blocks[0].shape[-1]
    cells = jnp.stack(returned, axis=0)
    cells = cells[jnp.stack([source(spot, jnp.int32(c), parts) if doubling(parts) else lax.rem(spot - c + parts, parts) for c in range(parts)])]
    cells = cells.reshape(rows, along // lanes, held, lanes)
    return cells.transpose(2, 0, 1, 3).reshape(tracers.shape)


def solution(mesh):
    placed = (
        P("trc", "tile", None, None),
        P(None, "tile", None, "trc"),
        P(None, "tile", None, "trc"),
        P(None, "tile", None, None),
        P(),
        P(),
        P(),
    )

    return jax.shard_map(
        on_device,
        mesh=mesh,
        in_specs=placed,
        out_specs=P("trc", "tile", None, None),
        check_vma=False,
    )
```
